32 devices in a mesh: row: 8 (over y, x, core), col: 4 (over z).
Axes of the slice: x: 2, y: 2, z: 4, core: 2. Of those that a mesh axis runs over, the one named last changes fastest.
Arguments:
- rotation: bfloat16 [8192, 8192], P('row', 'col'), may hold values from -0.0625 to 0.0625
- gradient: bfloat16 [8192, 8192], P('row', 'col'), may hold values from -0.0625 to 0.0625
Outputs:
- updated: float32 [8192, 2048], P('row', 'col')
- column_norms: float32 [2048], P('col')
The draws below stay inside these ranges and needn't reach their ends.
All inputs are finite; a program needn't handle non-finite values.
Results may differ from the reference program's by a relative error of at most 0.01.
Values may be sent and summed in bfloat16 or wider, within the bound.
No kernel may reach another device: no remote copies, remote signals or barrier semaphores. Data moves between devices by JAX's collectives and lax.ppermute only.
A program may use at most 128 MiB of HBM per device.

```python
import jax
import jax.numpy as jnp
from jax import lax

N = 8192
SLAB = 2048
N_ROW = 8


def levels(key, dims, split, least, high):
    level = 1.0
    for axis_at, blocks in split:
        steps = jax.random.uniform(jax.random.fold_in(jax.random.fold_in(key, 6), axis_at), (blocks,), jnp.float32, least / len(split), high / len(split))
        level = level * jnp.repeat(jnp.exp(steps), dims[axis_at] // blocks).reshape((-1,) + (1,) * (len(dims) - 1 - axis_at))
    return level


def normal_values(own_key, extent, width, most, cuts=(), kind=jnp.bfloat16):
    values = width * jax.random.normal(own_key, extent, jnp.float32)
    if cuts:
        values = values * levels(own_key, extent, cuts, -0.22, 0.18)
    return jnp.clip(values, -most, most).astype(kind)


def setup_inputs(seed: int = 0) -> dict:
    seeds = jax.random.split(jax.random.key(seed), 3)
    return {
        "rotation": normal_values(seeds[0], (N, N), N ** -0.5, 0.0625, ((0, 8), (1, 4))),
        "gradient": normal_values(seeds[1], (N, N), N ** -0.5, 0.0625, ((0, 8), (1, 4))),
    }


def apply_generator(rotation, gradient, panel):
    block = N // N_ROW
    rot_blocks = rotation.reshape(N_ROW, block, N)
    grad_blocks = gradient.reshape(N_ROW, block, N)
    pan_blocks = panel.reshape(N_ROW, block, panel.shape[1])

    def add_block(carry, pieces):
        rot_piece, grad_piece, pan_piece = pieces
        left = jnp.dot(rot_piece.T, pan_piece, preferred_element_type=jnp.float32)
        right = jnp.dot(grad_piece.T, pan_piece, preferred_element_type=jnp.float32)
        left = lax.optimization_barrier(left.astype(jnp.bfloat16)).astype(jnp.float32)
        right = lax.optimization_barrier(right.astype(jnp.bfloat16)).astype(jnp.float32)
        return ((carry[0] + left, carry[1] + right), None)
    zeros = jnp.zeros((N, panel.shape[1]), jnp.float32)
    (left_sum, right_sum), _ = lax.scan(add_block, (zeros, zeros), (rot_blocks, grad_blocks, pan_blocks))
    left_sum = left_sum.astype(jnp.bfloat16)
    right_sum = right_sum.astype(jnp.bfloat16)
    return jnp.dot(gradient, left_sum, preferred_element_type=jnp.float32) - jnp.dot(rotation, right_sum, preferred_element_type=jnp.float32)

def reference(rotation, gradient):
    base = rotation[:, ::N // SLAB]
    base_wide = base.astype(jnp.float32)
    first = base_wide + 0.25 * apply_generator(rotation, gradient, base)
    middle = (base_wide + first).astype(jnp.bfloat16)
    updated = base_wide + 0.125 * apply_generator(rotation, gradient, middle)
    column_norms = jnp.sqrt(lax.optimization_barrier(jnp.sum(updated * updated, axis=0)))
    return (updated, column_norms)
```

```python
import jax
import jax.numpy as jnp
from jax import lax
from jax.sharding import PartitionSpec as P

STRIDE = 4
SHARES = (4, 4, 4, 4)


f32, bf16 = jnp.float32, jnp.bfloat16


def mm(a, b):
    return lax.dot_general(a, b, (((1,), (0,)), ((), ())), preferred_element_type=f32)


def mm_t(a, b):
    return lax.dot_general(a, b, (((1,), (1,)), ((), ())), preferred_element_type=f32)


def tie(arrays, token):
    if token is None:
        return list(arrays)
    return list(lax.optimization_barrier((*arrays, token))[:-1])


def solution(mesh):
    rows, cols = mesh.shape["row"], mesh.shape["col"]
    bits = (rows // 2).bit_length() - 1
    blocks = 1 << bits
    sigmas = (tuple(range(bits)), tuple(range(bits))[::-1])
    orders = [
        sorted(range(blocks), key=lambda j, s=s: tuple(j >> b & 1 for b in s)) for s in sigmas
    ]

    def swap(v, mask):
        return lax.ppermute(v, "row", [(i, i ^ mask) for i in range(rows)])

    def turn(v, step):
        return lax.ppermute(v, "col", [(i, (i + step) % cols) for i in range(cols)])

    def on_device(rotation, gradient):
        me_row, me_col = lax.axis_index("row"), lax.axis_index("col")
        core, place = me_row % 2, me_row // 2
        local_rows, local_k = rotation.shape
        block = local_k // blocks
        count = local_k // STRIDE
        half = count // 2
        unit = half // sum(SHARES)
        edges = [0]
        for s in SHARES:
            edges.append(edges[-1] + s * unit)
        n = len(SHARES)

        t = lax.broadcasted_iota(jnp.int32, (count, local_k), 0)
        k = lax.broadcasted_iota(jnp.int32, (count, local_k), 1)
        pick = (k == STRIDE * ((t + half * core) % count)).astype(bf16)
        base_own = mm_t(pick, rotation).astype(bf16)
        base_other = base_own[half:]
        base = jnp.concatenate([base_own[:half], swap(base_other, 1)], axis=1)
        bases = [base[a:b] for a, b in zip(edges, edges[1:])]

        def spread(w, order):
            parts = [
                lax.dynamic_slice_in_dim(w, (j ^ place) * block, block, axis=1) for j in order
            ]
            own = lax.optimization_barrier(jnp.concatenate(parts, axis=1))
            return jnp.concatenate([own, swap(own, 1)], axis=0)

        weights = [spread(w, o) for w, o in zip((rotation, gradient), orders)]
        mid_k = local_k // 2

        state = [dict() for _ in range(2 * n)]
        token = [None]

        def step(k, arrays):
            return tie(arrays, token[0])

        def start_panel(k, own):
            state[k]["ups"], state[k]["downs"] = [own], [own]
            state[k]["ups"].append(turn(own, 1))
            if cols > 2:
                state[k]["downs"].append(turn(own, -1))

        def forward_panel(k):
            s = state[k]
            ups, downs = s["ups"], s["downs"]
            while len(ups) + len(downs) < cols + 1:
                if len(ups) <= len(downs):
                    ups.append(turn(ups[-1], 1))
                else:
                    downs.append(turn(downs[-1], -1))

        def multiply(k):
            s = state[k]
            if k < n:
                panel = lax.all_gather(bases[k], "col", axis=0, tiled=True)
                (panel,) = step(k, [panel])
            else:
                ups, downs = s["ups"], s["downs"]
                near = step(k, ups + downs[1:])
                ups, downs = near[: len(ups)], [None] + near[len(ups) :]
                def pick_piece(z, j):
                    d = (z - j) % cols
                    return ups[d] if d < len(ups) else downs[cols - d]

                panel = jnp.concatenate(
                    [
                        lax.select_n(me_col, *[pick_piece(z, j) for z in range(cols)])
                        for j in range(cols)
                    ],
                    axis=0,
                )
            sent = [mm(panel, w[:, mid_k:]).astype(bf16) for w in weights]
            s["recv"] = [swap(v, 2 << sg[0]) for v, sg in zip(sent, sigmas)]
            s["kept"] = [mm(panel, w[:, :mid_k]) for w in weights]
            token[0] = s["kept"][1]

        def add(k, t):
            s = state[k]
            recv = step(k, s["recv"])
            acc = [a + r.astype(f32) for a, r in zip(s["kept"], recv)]
            half_k = acc[0].shape[1] // 2
            if t + 1 < bits:
                sent = [a[:, half_k:].astype(bf16) for a in acc]
                s["recv"] = [swap(v, 2 << sg[t + 1]) for v, sg in zip(sent, sigmas)]
                s["kept"] = [a[:, :half_k] for a in acc]
                token[0] = sent[1]
            else:
                whole = [a.astype(bf16) for a in acc]
                s["part"] = [[w, swap(w, 2 << sg[t])] for w, sg in zip(whole, sigmas)]
                token[0] = whole[1]

        def widen(k, t):
            s = state[k]
            got = step(k, [p[1] for p in s["part"]])
            whole = [jnp.concatenate([p[0], g], axis=1) for p, g in zip(s["part"], got)]
            s["part"] = [[w, swap(w, 2 << sg[t])] for w, sg in zip(whole, sigmas)]
            token[0] = whole[1]

        def finish(k):
            s = state[k]
            got = step(k, [p[1] for p in s["part"]])
            full = []
            for i in (0, 1):
                pieces = [
                    p[:, a : a + block]
                    for p in (s["part"][i][0], got[i])
                    for a in range(0, p.shape[1], block)
                ]
                by_block = dict(zip(orders[i], pieces))
                full.append(jnp.concatenate([by_block[j] for j in orders[1 - i]], axis=1))
            term = (mm_t(full[0], weights[1]) - mm_t(full[1], weights[0])).astype(bf16)
            token[0] = term
            s["term"] = lax.psum_scatter(term, "col", scatter_dimension=0, tiled=True)

        def middle(k):
            (term,) = step(k, [state[k]["term"]])
            wide = bases[k].astype(f32)
            mid = (wide + (wide + 0.25 * term.astype(f32))).astype(bf16)
            token[0] = mid
            start_panel(k + n, mid)

        last = 2 * n
        for k in range(-3, last):
            if 0 <= k + 1 < last:
                add(k + 1, bits - 1)
            if 0 <= k < last:
                finish(k)
            if 0 <= k + 2 < last:
                for t in range(bits - 1):
                    add(k + 2, t)
            if 0 <= k + 1 < last:
                for t in range(bits - 2, -1, -1):
                    widen(k + 1, t)
            if n <= k + 3 < last:
                forward_panel(k + 3)
            if 0 <= k + 3 < last:
                multiply(k + 3)
            if 0 <= k < n:
                middle(k)

        terms = [state[k]["term"] for k in range(n, last)]
        ups = [b.astype(f32) + 0.125 * t.astype(f32) for b, t in zip(bases, terms)]
        squares = jnp.concatenate([jnp.sum(u * u, axis=1) for u in ups])
        mine = jnp.concatenate([u[:, :local_rows] for u in ups], axis=0)
        fetched = swap(jnp.concatenate([t[:, local_rows:] for t in terms], axis=0), 1)
        other = base_other.astype(f32) + 0.125 * fetched.astype(f32)
        low = jnp.where(core == 0, mine, other)
        high = jnp.where(core == 0, other, mine)
        updated = jnp.concatenate([low, high], axis=0).T
        blank = jnp.zeros_like(squares)
        placed = jnp.concatenate(
            [jnp.where(core == 0, squares, blank), jnp.where(core == 0, blank, squares)]
        )
        return (updated, jnp.sqrt(lax.psum(placed, "row")))

    return jax.shard_map(
        on_device,
        mesh=mesh,
        in_specs=(P("row", "col"), P("row", "col")),
        out_specs=(P("row", "col"), P("col")),
        check_vma=False,
    )
```

```python
import jax
import jax.numpy as jnp
from jax import lax
from jax.sharding import PartitionSpec as P


STRIDE = 4
SHARES = (4, 4, 4, 4)
GATHERED = (0, 1, 2, 3)
PLAN = (
    "B0", "C0", "B1", "D0", "C1", "E0", "B2", "D1", "F0", "C2", "B3", "D2",
    "E1", "C3", "E2", "G0", "F1", "D3", "A4", "F2", "E3", "B4", "G1", "F3",
    "C4", "A5", "D4", "G2", "B5", "E4", "A6", "C5", "G3", "B6", "D5", "F4",
    "A7", "C6", "E5", "B7", "D6", "F5", "C7", "E6", "D7", "F6", "E7", "F7",
)


f32, bf16 = jnp.float32, jnp.bfloat16


def mm(a, b):
    return lax.dot_general(a, b, (((1,), (0,)), ((), ())), preferred_element_type=f32)


def mm_t(a, b):
    return lax.dot_general(a, b, (((1,), (1,)), ((), ())), preferred_element_type=f32)


def tie(arrays, token):
    if token is None:
        return list(arrays)
    return list(lax.optimization_barrier((*arrays, token))[:-1])


def solution(mesh):
    rows, cols = mesh.shape["row"], mesh.shape["col"]
    bits = (rows // 2).bit_length() - 1
    blocks = 1 << bits
    sigmas = (tuple(range(bits)), tuple(range(bits))[::-1])
    orders = [
        sorted(range(blocks), key=lambda j, s=s: tuple(j >> b & 1 for b in s)) for s in sigmas
    ]

    def swap(v, mask):
        return lax.ppermute(v, "row", [(i, i ^ mask) for i in range(rows)])

    def turn(v, step):
        return lax.ppermute(v, "col", [(i, (i + step) % cols) for i in range(cols)])

    def on_device(rotation, gradient):
        me_row, me_col = lax.axis_index("row"), lax.axis_index("col")
        core, place = me_row % 2, me_row // 2
        local_rows, local_k = rotation.shape
        block = local_k // blocks
        count = local_k // STRIDE
        half = count // 2
        unit = half // sum(SHARES)
        edges = [0]
        for s in SHARES:
            edges.append(edges[-1] + s * unit)
        n = len(SHARES)

        t = lax.broadcasted_iota(jnp.int32, (count, local_k), 0)
        k = lax.broadcasted_iota(jnp.int32, (count, local_k), 1)
        pick = (k == STRIDE * ((t + half * core) % count)).astype(bf16)
        base_own = mm_t(pick, rotation).astype(bf16)
        base_other = base_own[half:]
        base = jnp.concatenate([base_own[:half], swap(base_other, 1)], axis=1)
        bases = [base[a:b] for a, b in zip(edges, edges[1:])]

        def spread(w, order):
            parts = [
                lax.dynamic_slice_in_dim(w, (j ^ place) * block, block, axis=1) for j in order
            ]
            own = lax.optimization_barrier(jnp.concatenate(parts, axis=1))
            return jnp.concatenate([own, swap(own, 1)], axis=0)

        x_late, g_late = tie([rotation, gradient], base_other)
        weights = [spread(w, o) for w, o in zip((x_late, g_late), orders)]
        turned = list(lax.optimization_barrier(tuple(w.T for w in weights)))
        token_start = turned[1]
        mid_k = local_k // 2

        state = [dict() for _ in range(2 * n)]
        token = [token_start]

        def step(arrays):
            return tie(arrays, token[0])

        def start_panel(k, own):
            state[k]["ups"], state[k]["downs"] = [own], [own]
            state[k]["ups"].append(turn(own, 1))
            if cols > 2:
                state[k]["downs"].append(turn(own, -1))

        def forward_panel(k):
            s = state[k]
            ups, downs = s["ups"], s["downs"]
            while len(ups) + len(downs) < cols + 1:
                if len(ups) <= len(downs):
                    ups.append(turn(ups[-1], 1))
                else:
                    downs.append(turn(downs[-1], -1))

        def multiply(k):
            s = state[k]
            if k in GATHERED:
                panel = lax.all_gather(bases[k], "col", axis=0, tiled=True)
                (panel,) = step([panel])
            else:
                ups, downs = s["ups"], s["downs"]
                near = step(ups + downs[1:])
                ups, downs = near[: len(ups)], [None] + near[len(ups) :]

                def pick_piece(z, j):
                    d = (z - j) % cols
                    return ups[d] if d < len(ups) else downs[cols - d]

                panel = jnp.concatenate(
                    [
                        lax.select_n(me_col, *[pick_piece(z, j) for z in range(cols)])
                        for j in range(cols)
                    ],
                    axis=0,
                )
            panel = lax.optimization_barrier(panel)
            sent = [mm(panel, w[:, mid_k:]).astype(bf16) for w in weights]
            s["recv"] = [swap(v, 2 << sg[0]) for v, sg in zip(sent, sigmas)]
            kept = [
                mm(tie([panel], v)[0], w[:, :mid_k]).astype(bf16)
                for w, v in zip(weights, sent)
            ]
            s["terms"] = [[v] for v in lax.optimization_barrier(tuple(kept))]
            token[0] = kept[1]

        def add(k, t):
            s = state[k]
            depth = len(s["terms"][0])
            flat = step(s["recv"] + s["terms"][0] + s["terms"][1])
            groups = [[flat[0], *flat[2 : 2 + depth]], [flat[1], *flat[2 + depth :]]]
            low = half_k = groups[0][0].shape[1]
            if t + 1 < bits:
                low = half_k // 2

            def total(group, a, b):
                return sum(v[:, a:b].astype(f32) for v in group[1:]) + group[0][:, a:b].astype(f32)

            if t + 1 < bits:
                sent = [total(group, low, half_k).astype(bf16) for group in groups]
                s["recv"] = [swap(v, 2 << sg[t + 1]) for v, sg in zip(sent, sigmas)]
                s["terms"] = groups
                token[0] = sent[1]
            else:
                whole = [total(group, 0, low).astype(bf16) for group in groups]
                s["part"] = [[w, swap(w, 2 << sg[t])] for w, sg in zip(whole, sigmas)]
                token[0] = whole[1]

        def widen(k, t):
            s = state[k]
            got = step([p[1] for p in s["part"]])
            whole = [jnp.concatenate([p[0], g], axis=1) for p, g in zip(s["part"], got)]
            s["part"] = [[w, swap(w, 2 << sg[t])] for w, sg in zip(whole, sigmas)]
            token[0] = whole[1]

        def finish(k):
            s = state[k]
            got = step([p[1] for p in s["part"]])
            full = []
            for i in (0, 1):
                pieces = [
                    p[:, a : a + block]
                    for p in (s["part"][i][0], got[i])
                    for a in range(0, p.shape[1], block)
                ]
                by_block = dict(zip(orders[i], pieces))
                full.append(jnp.concatenate([by_block[j] for j in orders[1 - i]], axis=1))
            full = lax.optimization_barrier(tuple(full))
            term = (mm(full[0], turned[1]) - mm(full[1], turned[0])).astype(bf16)
            token[0] = term
            s["term"] = lax.psum_scatter(term, "col", scatter_dimension=0, tiled=True)

        def middle(k):
            (term,) = step([state[k]["term"]])
            wide = bases[k].astype(f32)
            mid = (wide + (wide + 0.25 * term.astype(f32))).astype(bf16)
            token[0] = mid
            start_panel(k + n, mid)

        last = 2 * n

        def early(k):
            start_panel(k, bases[k])

        def sums(k):
            for t in range(bits - 1):
                add(k, t)

        def widens(k):
            for t in range(bits - 2, -1, -1):
                widen(k, t)

        steps = {
            "A": forward_panel,
            "B": multiply,
            "C": sums,
            "D": lambda k: add(k, bits - 1),
            "E": widens,
            "F": finish,
            "G": middle,
        }
        for k in range(n):
            if k not in GATHERED:
                early(k)
        for name in PLAN:
            steps[name[0]](int(name[1:]))

        terms = [state[k]["term"] for k in range(n, last)]
        ups = [b.astype(f32) + 0.125 * t.astype(f32) for b, t in zip(bases, terms)]
        squares = jnp.concatenate([jnp.sum(u * u, axis=1) for u in ups])
        mine = jnp.concatenate([u[:, :local_rows] for u in ups], axis=0)
        fetched = swap(jnp.concatenate([t[:, local_rows:] for t in terms], axis=0), 1)
        other = base_other.astype(f32) + 0.125 * fetched.astype(f32)
        low = jnp.where(core == 0, mine, other)
        high = jnp.where(core == 0, other, mine)
        updated = jnp.concatenate([low, high], axis=0).T
        squares = squares + sum(swap(squares, 2 * j) for j in range(1, blocks))
        pair = swap(squares, 1)
        norms = jnp.where(
            core == 0, jnp.concatenate([squares, pair]), jnp.concatenate([pair, squares])
        )
        return (updated, jnp.sqrt(norms))

    return jax.shard_map(
        on_device,
        mesh=mesh,
        in_specs=(P("row", "col"), P("row", "col")),
        out_specs=(P("row", "col"), P("col")),
        check_vma=False,
    )
```

```python
import jax
import jax.numpy as jnp
from jax import lax
from jax.sharding import PartitionSpec as P


STRIDE = 4
SHARES = (4, 4, 4, 4)
GATHERED = (0, 1, 2, 3)
PLAN = (
    "B0", "C0", "B1", "E0", "C1", "B2", "F0", "E1", "B3", "C2", "F1", "C3",
    "G0", "E2", "E3", "A4", "F2", "G1", "B4", "F3", "A5", "C4", "G2", "B5",
    "E4", "A6", "C5", "G3", "B6", "F4", "A7", "E5", "C6", "B7", "F5", "E6",
    "C7", "F6", "E7", "F7",
)


f32, bf16 = jnp.float32, jnp.bfloat16


def mm(a, b):
    return lax.dot_general(a, b, (((1,), (0,)), ((), ())), preferred_element_type=f32)


def mm_t(a, b):
    return lax.dot_general(a, b, (((1,), (1,)), ((), ())), preferred_element_type=f32)


def tie(arrays, token):
    if token is None:
        return list(arrays)
    return list(lax.optimization_barrier((*arrays, token))[:-1])


def solution(mesh):
    rows, cols = mesh.shape["row"], mesh.shape["col"]
    bits = (rows // 2).bit_length() - 1
    blocks = 1 << bits
    sigmas = (tuple(range(bits)), tuple(range(bits))[::-1])

    def swap(v, mask):
        return lax.ppermute(v, "row", [(i, i ^ mask) for i in range(rows)])

    def turn(v, step):
        return lax.ppermute(v, "col", [(i, (i + step) % cols) for i in range(cols)])

    def on_device(rotation, gradient):
        me_row, me_col = lax.axis_index("row"), lax.axis_index("col")
        core, place = me_row % 2, me_row // 2
        local_rows, local_k = rotation.shape
        count = local_k // STRIDE
        half = count // 2
        unit = half // sum(SHARES)
        edges = [0]
        for s in SHARES:
            edges.append(edges[-1] + s * unit)
        n = len(SHARES)

        t = lax.broadcasted_iota(jnp.int32, (count, local_k), 0)
        k = lax.broadcasted_iota(jnp.int32, (count, local_k), 1)
        pick = (k == STRIDE * ((t + half * core) % count)).astype(bf16)
        base_own = mm_t(pick, rotation).astype(bf16)
        base_other = base_own[half:]
        base = jnp.concatenate([base_own[:half], swap(base_other, 1)], axis=1)
        bases = [base[a:b] for a, b in zip(edges, edges[1:])]

        def spread(w, bit):
            parts = [
                lax.dynamic_slice_in_dim(w, (j ^ bit) * mid_k, mid_k, axis=1) for j in (0, 1)
            ]
            own = lax.optimization_barrier(jnp.concatenate(parts, axis=1))
            return jnp.concatenate([own, swap(own, 1)], axis=0)

        mid_k = local_k // 2
        ends = [place >> sg[0] & 1 for sg in sigmas]
        x_late, g_late = tie([rotation, gradient], base_other)
        weights = [spread(w, o) for w, o in zip((x_late, g_late), ends)]
        turned = list(lax.optimization_barrier(tuple(w.T for w in weights)))
        token_start = turned[1]

        state = [dict() for _ in range(2 * n)]
        token = [token_start]

        def step(arrays):
            return tie(arrays, token[0])

        def start_panel(k, own):
            state[k]["ups"], state[k]["downs"] = [own], [own]
            state[k]["ups"].append(turn(own, 1))
            if cols > 2:
                state[k]["downs"].append(turn(own, -1))

        def forward_panel(k):
            s = state[k]
            ups, downs = s["ups"], s["downs"]
            while len(ups) + len(downs) < cols + 1:
                if len(ups) <= len(downs):
                    ups.append(turn(ups[-1], 1))
                else:
                    downs.append(turn(downs[-1], -1))

        def multiply(k):
            s = state[k]
            if k in GATHERED:
                panel = lax.all_gather(bases[k], "col", axis=0, tiled=True)
                (panel,) = step([panel])
            else:
                ups, downs = s["ups"], s["downs"]
                near = step(ups + downs[1:])
                ups, downs = near[: len(ups)], [None] + near[len(ups) :]

                def pick_piece(z, j):
                    d = (z - j) % cols
                    return ups[d] if d < len(ups) else downs[cols - d]

                panel = jnp.concatenate(
                    [
                        lax.select_n(me_col, *[pick_piece(z, j) for z in range(cols)])
                        for j in range(cols)
                    ],
                    axis=0,
                )
            panel = lax.optimization_barrier(panel)
            sent = [mm(panel, w[:, mid_k:]).astype(bf16) for w in weights]
            s["recv"] = [swap(v, 2 << sg[0]) for v, sg in zip(sent, sigmas)]
            kept = [
                mm(tie([panel], v)[0], w[:, :mid_k]).astype(bf16)
                for w, v in zip(weights, sent)
            ]
            s["kept"] = list(lax.optimization_barrier(tuple(kept)))
            token[0] = kept[1]

        def exchange(k, t):
            s = state[k]
            flat = step(s["recv"] + s["kept"])
            sums = [(flat[i].astype(f32) + flat[2 + i].astype(f32)).astype(bf16) for i in (0, 1)]
            s["recv"] = [swap(v, 2 << sg[t]) for v, sg in zip(sums, sigmas)]
            s["kept"] = sums
            token[0] = sums[1]

        def finish(k):
            s = state[k]
            flat = step(s["recv"] + s["kept"])
            same = ends[0] == ends[1]
            full = [
                jnp.concatenate(
                    [jnp.where(same, own, got), jnp.where(same, got, own)], axis=1
                )
                for got, own in zip(flat[:2], flat[2:])
            ]
            full = lax.optimization_barrier(tuple(full))
            term = (mm(full[0], turned[1]) - mm(full[1], turned[0])).astype(bf16)
            token[0] = term
            s["term"] = lax.psum_scatter(term, "col", scatter_dimension=0, tiled=True)

        def middle(k):
            (term,) = step([state[k]["term"]])
            wide = bases[k].astype(f32)
            mid = (wide + (wide + 0.25 * term.astype(f32))).astype(bf16)
            token[0] = mid
            start_panel(k + n, mid)

        last = 2 * n

        def early(k):
            start_panel(k, bases[k])

        def middles(k):
            for t in range(1, bits):
                exchange(k, t)

        steps = {
            "A": forward_panel,
            "B": multiply,
            "C": middles,
            "E": lambda k: exchange(k, 0),
            "F": finish,
            "G": middle,
        }
        for k in range(n):
            if k not in GATHERED:
                early(k)
        for name in PLAN:
            steps[name[0]](int(name[1:]))

        terms = [state[k]["term"] for k in range(n, last)]
        ups = [b.astype(f32) + 0.125 * t.astype(f32) for b, t in zip(bases, terms)]
        squares = jnp.concatenate([jnp.sum(u * u, axis=1) for u in ups])
        mine = jnp.concatenate([u[:, :local_rows] for u in ups], axis=0)
        fetched = swap(jnp.concatenate([t[:, local_rows:] for t in terms], axis=0), 1)
        other = base_other.astype(f32) + 0.125 * fetched.astype(f32)
        low = jnp.where(core == 0, mine, other)
        high = jnp.where(core == 0, other, mine)
        updated = jnp.concatenate([low, high], axis=0).T
        squares = squares + sum(swap(squares, 2 * j) for j in range(1, blocks))
        pair = swap(squares, 1)
        norms = jnp.where(
            core == 0, jnp.concatenate([squares, pair]), jnp.concatenate([pair, squares])
        )
        return (updated, jnp.sqrt(norms))

    return jax.shard_map(
        on_device,
        mesh=mesh,
        in_specs=(P("row", "col"), P("row", "col")),
        out_specs=(P("row", "col"), P("col")),
        check_vma=False,
    )
```

```python
import jax
import jax.numpy as jnp
from jax import lax
from jax.sharding import PartitionSpec as P


STRIDE = 4
SHARES = (4, 4, 4, 4)
GATHERED = (0, 1, 2, 3)
PLAN = (
    "B0", "C0", "B1", "E0", "C1", "B2", "F0", "E1", "B3", "H0", "C2", "F1",
    "C3", "G0", "E2", "H1", "E3", "A4", "F2", "G1", "B4", "H2", "F3", "A5",
    "C4", "G2", "B5", "H3", "E4", "A6", "C5", "G3", "B6", "F4", "A7", "E5",
    "C6", "B7", "F5", "E6", "C7", "F6", "E7", "F7",
)


f32, bf16 = jnp.float32, jnp.bfloat16


def mm(a, b):
    return lax.dot_general(a, b, (((1,), (0,)), ((), ())), preferred_element_type=f32)


def mm_t(a, b):
    return lax.dot_general(a, b, (((1,), (1,)), ((), ())), preferred_element_type=f32)


def tie(arrays, token):
    if token is None:
        return list(arrays)
    return list(lax.optimization_barrier((*arrays, token))[:-1])


def solution(mesh):
    rows, cols = mesh.shape["row"], mesh.shape["col"]
    bits = (rows // 2).bit_length() - 1
    blocks = 1 << bits
    sigmas = (tuple(range(bits)), tuple(range(bits))[::-1])

    def swap(v, mask):
        return lax.ppermute(v, "row", [(i, i ^ mask) for i in range(rows)])

    def swap_col(v, mask):
        return lax.ppermute(v, "col", [(i, i ^ mask) for i in range(cols)])

    masks = [1 << b for b in range(cols.bit_length() - 1)][::-1]

    def on_device(rotation, gradient):
        me_row, me_col = lax.axis_index("row"), lax.axis_index("col")
        core, place = me_row % 2, me_row // 2
        local_rows, local_k = rotation.shape
        count = local_k // STRIDE
        half = count // 2
        unit = half // sum(SHARES)
        edges = [0]
        for s in SHARES:
            edges.append(edges[-1] + s * unit)
        n = len(SHARES)

        t = lax.broadcasted_iota(jnp.int32, (count, local_k), 0)
        k = lax.broadcasted_iota(jnp.int32, (count, local_k), 1)
        pick = (k == STRIDE * ((t + half * core) % count)).astype(bf16)
        base_own = mm_t(pick, rotation).astype(bf16)
        base_other = base_own[half:]
        base = jnp.concatenate([base_own[:half], swap(base_other, 1)], axis=1)
        bases = [base[a:b] for a, b in zip(edges, edges[1:])]

        def spread(w, bit):
            parts = [
                lax.dynamic_slice_in_dim(w, (j ^ bit) * mid_k, mid_k, axis=1) for j in (0, 1)
            ]
            own = lax.optimization_barrier(jnp.concatenate(parts, axis=1))
            return jnp.concatenate([own, swap(own, 1)], axis=0)

        mid_k = local_k // 2
        ends = [place >> sg[0] & 1 for sg in sigmas]
        x_late, g_late = tie([rotation, gradient], base_other)
        weights = [spread(w, o) for w, o in zip((x_late, g_late), ends)]
        turned = list(lax.optimization_barrier(tuple(w.T for w in weights)))
        token_start = turned[1]

        state = [dict() for _ in range(2 * n)]
        token = [token_start]

        def step(arrays):
            return tie(arrays, token[0])

        def start_panel(k, own):
            state[k]["own"] = own
            state[k]["pieces"] = {m: swap_col(own, m) for m in masks}

        def forward_panel(k):
            pieces = state[k]["pieces"]
            for m in masks:
                for low in [d for d in pieces if d & -d > m]:
                    if low | m not in pieces:
                        pieces[low | m] = swap_col(pieces[low], m)

        def multiply(k):
            s = state[k]
            if k in GATHERED:
                panel = lax.all_gather(bases[k], "col", axis=0, tiled=True)
                (panel,) = step([panel])
            else:
                offsets = sorted(s["pieces"])
                near = step([s["own"]] + [s["pieces"][d] for d in offsets])
                panel = jnp.concatenate(
                    [
                        lax.select_n(me_col, *[near[z ^ j] for z in range(cols)])
                        for j in range(cols)
                    ],
                    axis=0,
                )
            panel = lax.optimization_barrier(panel)
            sent = [mm(panel, w[:, mid_k:]).astype(bf16) for w in weights]
            s["recv"] = [swap(v, 2 << sg[0]) for v, sg in zip(sent, sigmas)]
            kept = [
                mm(tie([panel], v)[0], w[:, :mid_k]).astype(bf16)
                for w, v in zip(weights, sent)
            ]
            s["kept"] = list(lax.optimization_barrier(tuple(kept)))
            token[0] = kept[1]

        def exchange(k, t):
            s = state[k]
            flat = step(s["recv"] + s["kept"])
            sums = [(flat[i].astype(f32) + flat[2 + i].astype(f32)).astype(bf16) for i in (0, 1)]
            s["recv"] = [swap(v, 2 << sg[t]) for v, sg in zip(sums, sigmas)]
            s["kept"] = sums
            token[0] = sums[1]

        def finish(k):
            s = state[k]
            flat = step(s["recv"] + s["kept"])
            same = ends[0] == ends[1]
            full = [
                jnp.concatenate(
                    [jnp.where(same, own, got), jnp.where(same, got, own)], axis=1
                )
                for got, own in zip(flat[:2], flat[2:])
            ]
            full = lax.optimization_barrier(tuple(full))
            term = (mm(full[0], turned[1]) - mm(full[1], turned[0])).astype(bf16)
            token[0] = term
            if k >= n:
                s["term"] = lax.psum_scatter(term, "col", scatter_dimension=0, tiled=True)
                return
            wide = term.shape[0] // cols
            s["rest"] = {
                d: [lax.dynamic_slice_in_dim(term, (me_col ^ d) * wide, wide, axis=0)]
                for d in range(cols)
            }
            hand_over(k, masks[-1])

        def total(parts):
            return sum(p.astype(f32) for p in parts)

        def hand_over(k, m):
            rest = state[k]["rest"]
            gone = [d for d in sorted(rest) if d & m]
            sent = jnp.concatenate([total(rest.pop(d)).astype(bf16) for d in gone], axis=0)
            state[k]["came"] = (gone, m, swap_col(sent, m))
            token[0] = sent

        def take(k):
            s = state[k]
            gone, m, got = s["came"]
            (got,) = step([got])
            wide = got.shape[0] // len(gone)
            for i, d in enumerate(gone):
                s["rest"][d ^ m].append(got[i * wide : (i + 1) * wide])

        def halve(k):
            for m in masks[-2::-1]:
                take(k)
                hand_over(k, m)

        def middle(k):
            take(k)
            wide = bases[k].astype(f32)
            mid = (wide + (wide + 0.25 * total(state[k]["rest"][0]))).astype(bf16)
            token[0] = mid
            start_panel(k + n, mid)

        last = 2 * n

        def early(k):
            start_panel(k, bases[k])

        def middles(k):
            for t in range(1, bits):
                exchange(k, t)

        steps = {
            "A": forward_panel,
            "B": multiply,
            "C": middles,
            "E": lambda k: exchange(k, 0),
            "F": finish,
            "G": middle,
            "H": halve,
        }
        for k in range(n):
            if k not in GATHERED:
                early(k)
        for name in PLAN:
            steps[name[0]](int(name[1:]))

        terms = [state[k]["term"] for k in range(n, last)]
        ups = [b.astype(f32) + 0.125 * t.astype(f32) for b, t in zip(bases, terms)]
        squares = jnp.concatenate([jnp.sum(u * u, axis=1) for u in ups])
        mine = jnp.concatenate([u[:, :local_rows] for u in ups], axis=0)
        fetched = swap(jnp.concatenate([t[:, local_rows:] for t in terms], axis=0), 1)
        other = base_other.astype(f32) + 0.125 * fetched.astype(f32)
        low = jnp.where(core == 0, mine, other)
        high = jnp.where(core == 0, other, mine)
        updated = jnp.concatenate([low, high], axis=0).T
        squares = squares + sum(swap(squares, 2 * j) for j in range(1, blocks))
        pair = swap(squares, 1)
        norms = jnp.where(
            core == 0, jnp.concatenate([squares, pair]), jnp.concatenate([pair, squares])
        )
        return (updated, jnp.sqrt(norms))

    return jax.shard_map(
        on_device,
        mesh=mesh,
        in_specs=(P("row", "col"), P("row", "col")),
        out_specs=(P("row", "col"), P("col")),
        check_vma=False,
    )
```
